32 devices in a mesh: replica: 1, ctx: 32 (over z, y, x, core).
Axes of the slice: x: 2, y: 2, z: 4, core: 2. Of those that a mesh axis runs over, the one named last changes fastest.
Arguments:
- queries: bfloat16 [128, 4096], P(('replica', 'ctx')), may hold values from -4 to 6.2
- own_key: bfloat16 [128, 256], P(('replica', 'ctx')), may hold values from -12 to 12
- own_value: bfloat16 [128, 256], P(('replica', 'ctx')), may hold values from -40 to 40
- cache_keys: bfloat16 [2, 1024, 256], P('replica', 'ctx'), may hold values from -4 to 4.7
- cache_values: bfloat16 [2, 1024, 256], P('replica', 'ctx'), may hold values from -40 to 40
- prefix_of_row: int32 [128], P('replica'), may hold values from 0 to 1, as said below
- context_len: int32 [2], P('replica'), may hold values from 512 to 1024
- hidden_in: bfloat16 [128, 4096], P(('replica', 'ctx')), may hold values from -3 to 3
- w_out: bfloat16 [4096, 4096], P('ctx'), may hold values from -0.09375 to 0.09375
- norm_gain: float32 [4096], replicated, may hold values from 0.5 to 1.5
- expert_ids: int32 [128, 8], P(('replica', 'ctx')), may hold values from 0 to 15, all different within a row; in each aligned block of 4 rows (0 to 3, 4 to 7, ...) at most 4 rows name the same one
- route_weights: float32 [128, 8], P(('replica', 'ctx')), may hold values from 0.05 to 0.4
- gate_up_codes: bfloat16 [32, 4096, 768], P('ctx'), may hold values from -0.09375 to 0.09375
- gate_up_scales: float32 [32, 32, 6], P('ctx'), may hold values from 0.6 to 1.7
- down_codes: bfloat16 [32, 384, 4096], P('ctx'), may hold values from -0.21875 to 0.21875
- down_scales: float32 [32, 3, 32], P('ctx'), may hold values from 0.6 to 1.7
Outputs:
- attention_out: bfloat16 [128, 4096], P(('replica', 'ctx'))
- layer_out: bfloat16 [128, 4096], P(('replica', 'ctx'))
The draws below stay inside these ranges and needn't reach their ends.
Inputs may be any that keep to these rules, and one draw needn't show every extreme that they name: `prefix_of_row`: the rows come in aligned blocks of 64 consecutive rows that all name one prefix. `expert_ids`: each row names 8 different experts; among the 4 rows of one device no expert is named more than 4 times.
All inputs are finite; a program needn't handle non-finite values.
Results may differ from the reference program's by a relative error of at most 0.014.
Values may be sent and summed in bfloat16 or wider, within the bound.
A program may use at most 128 MiB of HBM per device.

```python
import math
import jax
import jax.numpy as jnp
import numpy as np
from jax import lax

D = 4096
QH = 32
KVH = 2
HD = 128
CTX_DEV = 32
CAND = 64
ROW_DEV = 4
TOP = 8
EXP_HID = 768
BLK = 128
DQ = 4096
DKV = 256
CTX = 1024
ROWS = 128
PREFIXES = 2
EXPERTS = 16
CAP = 4
N_CTX = 32


def draw_queries(key, part):
    key_base = jax.random.fold_in(jax.random.fold_in(key, 11), 0)
    drawn = jnp.clip(jax.random.normal(key_base, (ROWS, QH * HD), jnp.float32), -4.0, 4.0)
    return drawn.astype(jnp.bfloat16)


def draw_cache_keys(key, part):
    key_base = jax.random.fold_in(jax.random.fold_in(key, 23), 0)
    drawn = jnp.clip(jax.random.normal(key_base, (PREFIXES, CTX, KVH * HD), jnp.float32), -4.0, 4.0)
    return drawn.astype(jnp.bfloat16)


def draw_prefix_of_row(key, part):
    block_choice = jax.random.randint(jax.random.fold_in(key, 37), (PREFIXES,), 0, PREFIXES).astype(jnp.int32)
    block_of_row = (jnp.arange(ROWS, dtype=jnp.int32) // CAND).astype(jnp.int32)
    return jnp.take(block_choice, block_of_row).astype(jnp.int32)


def levels(stream_key, shape, cuts, smallest, top_value):
    loudness = 1.0
    for dim, blocks in cuts:
        draws = jax.random.uniform(jax.random.fold_in(jax.random.fold_in(stream_key, 6), dim), (blocks,), jnp.float32, smallest / len(cuts), top_value / len(cuts))
        loudness = loudness * jnp.repeat(jnp.exp(draws), shape[dim] // blocks).reshape((-1,) + (1,) * (len(shape) - 1 - dim))
    return loudness


def assign_block(stream_key, own, number, rows, number_of, top, limit, slope):
    order = jax.random.permutation(stream_key, number_of)
    heavy_load, usual = shares(number_of, rows * top, limit, slope, True), shares(number_of, rows * top, limit, slope, False)
    places = jnp.arange(number_of)

    def named(sizes, turn):
        used = int((sizes > 0).sum())
        fixed = max(1, used // 4)
        passed = fixed + (places - fixed + turn * (used - fixed)) % max(1, number_of - fixed)
        return jnp.zeros((number_of,), jnp.int32).at[order[jnp.where(places < fixed, places, passed)]].set(jnp.asarray(sizes, jnp.int32))

    sizes = jnp.where(number % 4 == 0, named(heavy_load, number // 4), named(usual, number - number // 4 - 1))
    mixed = jax.random.permutation(jax.random.fold_in(own, 3), number_of)
    source_of, receiver = mixed[0:number_of // 2 * 2:2], mixed[1:number_of // 2 * 2:2]
    slack = jnp.minimum(sizes[source_of] - 1, limit - sizes[receiver]) // 2
    slack = jnp.where((source_of == order[0]) | (receiver == order[0]) | (sizes[receiver] == 0), 0, jnp.maximum(slack, 0))
    passed = jax.random.randint(jax.random.fold_in(own, 4), (number_of // 2,), 0, 1 << 20) % (slack + 1)
    sizes = sizes.at[source_of].add(-passed).at[receiver].add(passed)
    labels = jnp.searchsorted(jnp.cumsum(sizes), jnp.arange(rows * top), side="right").astype(jnp.int32)
    grid = labels.reshape(top, rows).T
    grid = grid[jax.random.permutation(jax.random.fold_in(own, 1), rows)]
    turn = jax.random.randint(jax.random.fold_in(own, 2), (rows, 1), 0, top)
    return jnp.take_along_axis(grid, (jnp.arange(top)[None, :] + turn) % top, axis=1)


def shares(number_of, total, limit, skew, full):
    loads = [(1 << 20) // math.isqrt(rank ** skew) + 1 for rank in range(1, number_of + 1)]
    largest = limit if full else min(limit, max(-(-total // number_of), total * loads[0] // sum(loads)))
    least = 1 if total - largest >= number_of - 1 else 0
    given, surplus = [largest] + [least] * (number_of - 1), total - largest - least * (number_of - 1)
    while surplus > 0:
        candidates = [i for i in range(1, number_of) if given[i] < largest] or [i for i in range(1, number_of) if given[i] < limit]
        whole, budget = sum([loads[i] for i in candidates]), surplus
        for i in candidates:
            more = min(limit - given[i], max(1, budget * loads[i] // whole), surplus)
            given[i] = given[i] + more
            surplus = surplus - more
    return np.array(given)


def bell_draw(key, dims, width, bound, cuts=(), kind=jnp.bfloat16):
    array = jax.random.normal(key, dims, jnp.float32) * width
    if len(cuts) > 0:
        array = levels(key, dims, cuts, -0.22, 0.18) * array
    return jnp.clip(array, min=-bound, max=bound).astype(kind)


def setup_inputs(seed: int = 0, part: int = 0) -> dict:
    key_of = jax.random.split(jax.random.key(seed), 17)
    part_splits = jax.random.split(jax.random.fold_in(key_of[16], part), 17)
    queries = draw_queries(jax.random.fold_in(jax.random.fold_in(key_of[16], part), 71), part)
    own_key = bell_draw(part_splits[1], (ROWS, DKV), 3.0, 12.0, ((0, 32),))
    own_value = bell_draw(part_splits[2], (ROWS, DKV), 8.0, 40.0, ((0, 32),))
    cache_keys = draw_cache_keys(jax.random.fold_in(jax.random.fold_in(key_of[16], part), 71), part)
    cache_values = bell_draw(part_splits[4], (PREFIXES, CTX, DKV), 8.0, 40.0, ((1, 32),))
    prefix_of_row = draw_prefix_of_row(jax.random.fold_in(jax.random.fold_in(key_of[16], part), 71), part)
    context_len = jax.random.randint(part_splits[6], (PREFIXES,), CTX // 2, CTX + 1).astype(jnp.int32)
    hidden_in = bell_draw(part_splits[7], (ROWS, D), 0.5, 3.0, ((0, 32),))
    w_out = bell_draw(key_of[8], (DQ, D), DQ ** -0.5, 0.09375, ((0, 32),))
    norm_gain = jnp.clip(1.0 + 0.1 * jax.random.normal(key_of[9], (D,), jnp.float32), 0.5, 1.5)
    expert_ids_keys = jax.random.split(jax.random.fold_in(part_splits[10], 1), ROWS // ROW_DEV)
    expert_ids_turns = jax.random.permutation(jax.random.fold_in(part_splits[10], 3), ROWS // ROW_DEV)
    expert_ids = jax.vmap(lambda own, number: assign_block(jax.random.fold_in(part_splits[10], 2), own, number, ROW_DEV, EXPERTS, TOP, CAP, 2))(expert_ids_keys, expert_ids_turns).reshape((ROWS, TOP))
    route_weights = jnp.clip(jnp.exp(math.log(0.4) - 2.0794415 * jax.random.uniform(part_splits[11], (ROWS, TOP), jnp.float32) ** levels(part_splits[11], (ROWS, TOP), ((0, 32),), -0.2, 0.2)), 0.05, 0.4)
    gate_up_codes = bell_draw(key_of[12], (2 * EXPERTS, D, EXP_HID), D ** -0.5, 0.09375, ((0, 32),))
    gate_up_scales = jnp.clip(jnp.exp(math.log(1.7) - 1.04145386 * jax.random.uniform(key_of[13], (2 * EXPERTS, D // BLK, EXP_HID // BLK), jnp.float32) ** levels(key_of[13], (2 * EXPERTS, D // BLK, EXP_HID // BLK), ((0, 32),), -0.2, 0.2)), 0.6, 1.7)
    down_codes = bell_draw(key_of[14], (2 * EXPERTS, EXP_HID // 2, D), EXP_HID ** -0.5, 0.21875, ((0, 32),))
    down_scales = jnp.clip(jnp.exp(math.log(1.7) - 1.04145386 * jax.random.uniform(key_of[15], (2 * EXPERTS, EXP_HID // (2 * BLK), D // BLK), jnp.float32) ** levels(key_of[15], (2 * EXPERTS, EXP_HID // (2 * BLK), D // BLK), ((0, 32),), -0.2, 0.2)), 0.6, 1.7)
    return dict(queries=queries, own_key=own_key, own_value=own_value, cache_keys=cache_keys, cache_values=cache_values, prefix_of_row=prefix_of_row, context_len=context_len, hidden_in=hidden_in, w_out=w_out, norm_gain=norm_gain, expert_ids=expert_ids, route_weights=route_weights, gate_up_codes=gate_up_codes, gate_up_scales=gate_up_scales, down_codes=down_codes, down_scales=down_scales)


NEG = -1e+30
EPSILON = 1e-06

def dequantize(code_values, scales):
    rows_per = code_values.shape[0] // scales.shape[0]
    cols_per = code_values.shape[1] // scales.shape[1]
    spread = jnp.repeat(jnp.repeat(scales, rows_per, axis=0), cols_per, axis=1)
    return (code_values.astype(jnp.float32) * spread).astype(jnp.bfloat16)

def reference(queries, own_key, own_value, cache_keys, cache_values, prefix_of_row, context_len, hidden_in, w_out, norm_gain, expert_ids, route_weights, gate_up_codes, gate_up_scales, down_codes, down_scales):
    row_total = queries.shape[0]
    per_group = QH // KVH
    score_scale = 1.0 / math.sqrt(HD)
    position = jnp.arange(CTX, dtype=jnp.int32).reshape(N_CTX, CTX_DEV)

    def attend_row(row_index):
        prefix = prefix_of_row[row_index]
        length = context_len[prefix]
        key_block = cache_keys[prefix].astype(jnp.float32).reshape(N_CTX, CTX_DEV, KVH, HD)
        values = cache_values[prefix].astype(jnp.float32).reshape(N_CTX, CTX_DEV, KVH, HD)
        query_heads = queries[row_index].astype(jnp.float32).reshape(KVH, per_group, HD)
        scores = jnp.einsum('gqd,ctgd->cgqt', query_heads, key_block) * score_scale
        is_valid = (position < length)[:, None, None, :]
        masked = jnp.where(is_valid, scores, NEG)
        block_max = lax.optimization_barrier(jnp.max(masked, axis=-1))
        weights = jnp.where(is_valid, jnp.exp(masked - block_max[..., None]), 0.0)
        block_total = lax.optimization_barrier(jnp.sum(weights, axis=-1))
        rounded = lax.optimization_barrier(weights.astype(jnp.bfloat16)).astype(jnp.float32)
        numerator = jnp.einsum('cgqt,ctgd->cgqd', rounded, values)
        block_out = numerator / jnp.maximum(block_total, 1.0)[..., None]
        block_out = lax.optimization_barrier(block_out.astype(jnp.bfloat16)).astype(jnp.float32)
        own_keys = own_key[row_index].astype(jnp.float32).reshape(KVH, HD)
        own_score = jnp.einsum('gqd,gd->gq', query_heads, own_keys) * score_scale
        top_score = jnp.maximum(lax.optimization_barrier(jnp.max(block_max, axis=0)), own_score)
        factor = block_total * jnp.exp(block_max - top_score[None])
        own_weight = jnp.exp(own_score - top_score)
        own_values = own_value[row_index].astype(jnp.float32).reshape(KVH, 1, HD)
        numerator_all = lax.optimization_barrier(jnp.sum(factor[..., None] * block_out, axis=0)) + own_weight[..., None] * own_values
        denominator = lax.optimization_barrier(jnp.sum(factor, axis=0)) + own_weight
        return (numerator_all / denominator[..., None]).reshape(QH * HD).astype(jnp.bfloat16)
    attended = lax.map(attend_row, jnp.arange(row_total, dtype=jnp.int32))
    mixed = hidden_in.astype(jnp.float32) + jnp.dot(attended, w_out, preferred_element_type=jnp.float32)
    attention_out = mixed.astype(jnp.bfloat16)
    mean_square = lax.optimization_barrier(jnp.mean(mixed * mixed, axis=-1, keepdims=True))
    normed = (mixed * lax.rsqrt(mean_square + EPSILON) * norm_gain).astype(jnp.bfloat16)
    pick_ids = expert_ids.reshape(-1).astype(jnp.int32)
    pick_count = pick_ids.shape[0]
    pick_row = (jnp.arange(pick_count, dtype=jnp.int32) // TOP).astype(jnp.int32)
    pick_weight = route_weights.reshape(-1)
    sorted_picks = jnp.argsort(pick_ids, stable=True).astype(jnp.int32)
    counts = lax.optimization_barrier(jnp.sum((pick_ids[None, :] == jnp.arange(EXPERTS, dtype=jnp.int32)[:, None]).astype(jnp.int32), axis=1))
    starts = (jnp.cumsum(counts) - counts).astype(jnp.int32)
    window = N_CTX * CAP
    padded_order = jnp.concatenate([sorted_picks, jnp.zeros((window,), jnp.int32)])
    half_width = EXP_HID // 2

    def add_expert(expert, running):
        chosen = lax.dynamic_slice_in_dim(padded_order, starts[expert], window)
        is_live = jnp.arange(window, dtype=jnp.int32) < counts[expert]
        inputs = normed[pick_row[chosen]]
        result = jnp.zeros((window, D), jnp.float32)
        for part_half in range(2):
            entry = 2 * expert + part_half
            gate_up = dequantize(lax.dynamic_index_in_dim(gate_up_codes, entry, 0, False), lax.dynamic_index_in_dim(gate_up_scales, entry, 0, False))
            down_proj = dequantize(lax.dynamic_index_in_dim(down_codes, entry, 0, False), lax.dynamic_index_in_dim(down_scales, entry, 0, False))
            projected_in = jnp.dot(inputs, gate_up, preferred_element_type=jnp.float32)
            activated = (jax.nn.silu(projected_in[:, :half_width]) * projected_in[:, half_width:]).astype(jnp.bfloat16)
            piece_out = jnp.dot(activated, down_proj, preferred_element_type=jnp.float32)
            result = result + lax.optimization_barrier(piece_out.astype(jnp.bfloat16)).astype(jnp.float32)
        scaled = jnp.where(is_live, pick_weight[chosen], 0.0)[:, None] * result
        return running.at[pick_row[chosen]].add(scaled)
    expert_sum = lax.fori_loop(0, EXPERTS, add_expert, jnp.zeros((row_total, D), jnp.float32))
    layer_out = (mixed + expert_sum).astype(jnp.bfloat16)
    return (attention_out, layer_out)
```

```python
import math

import jax
import jax.numpy as jnp
from jax import lax
from jax.experimental import pallas as pl
from jax.experimental.pallas import tpu as pltpu
from jax.sharding import PartitionSpec as P

HD = 128
CAND = 64


NEG = -1e30
EPSILON = 1e-06


def swapped(value, axis, distance):
    return lax.ppermute(value, axis, [(i, i ^ 1 << distance) for i in range(lax.axis_size(axis))])


def dequantize(code_values, scales):
    rows_per = code_values.shape[0] // scales.shape[0]
    cols_per = code_values.shape[1] // scales.shape[1]
    spread = jnp.repeat(jnp.repeat(scales, rows_per, axis=0), cols_per, axis=1)
    return (code_values.astype(jnp.float32) * spread).astype(jnp.bfloat16)


def block_partials(query_heads, key_heads, value_heads, is_valid, score_scale):
    scores = (
        jnp.einsum(
            "brgqd,bstgd->brgqst", query_heads, key_heads, preferred_element_type=jnp.float32
        )
        * score_scale
    )
    valid_full = is_valid[:, None, None, None, :, :]
    masked = jnp.where(valid_full, scores, NEG)
    block_max = jnp.max(masked, axis=-1)
    weights = jnp.where(valid_full, jnp.exp(masked - block_max[..., None]), 0.0)
    block_total = jnp.sum(weights, axis=-1)
    numerator = jnp.einsum(
        "brgqst,bstgd->brgqsd",
        weights.astype(jnp.bfloat16),
        value_heads,
        preferred_element_type=jnp.float32,
    )
    block_out = (numerator / jnp.maximum(block_total, 1.0)[..., None]).astype(jnp.bfloat16)
    return (block_max, block_total, block_out)


def fold_blocks(block_max, block_total, block_out):
    local_top = jnp.max(block_max, axis=-1)
    factor = block_total * jnp.exp(block_max - local_top[..., None])
    numer = jnp.sum(factor[..., None] * block_out.astype(jnp.float32), axis=-2)
    denom = jnp.sum(factor, axis=-1)
    return (local_top, numer, denom)


def merge_pair(first, second):
    top = jnp.maximum(first[0], second[0])
    scale_first = jnp.exp(first[0] - top)
    scale_second = jnp.exp(second[0] - top)
    numer = first[1] * scale_first[..., None] + second[1] * scale_second[..., None]
    denom = first[2] * scale_first + second[2] * scale_second
    return (top, numer, denom)


def flipped(index, pattern, bits):
    total = 0
    for bit in range(bits):
        value = index // (1 << bit) % 2
        if pattern >> bit & 1:
            value = 1 - value
        total = total + value * (1 << bit)
    return total


def greet(me, bits):
    barrier = pltpu.get_barrier_semaphore()
    for bit in range(bits):
        pl.semaphore_signal(
            barrier,
            inc=1,
            device_id={"ctx": flipped(me, 1 << bit, bits)},
            device_id_type=pl.DeviceIdType.MESH,
        )
    pl.semaphore_wait(barrier, bits)


def lane_parts(rows, bits):
    middle = rows // 32 * 16
    first = list(range(bits))
    second = list(range(bits))
    if bits > 2:
        second[1], second[2] = second[2], second[1]
    return ((0, middle, first), (middle, rows - middle, second))


def gather_kernel(bits, block_ref, out_ref, send_sem, recv_sem, own_sem):
    me = lax.axis_index("ctx")
    parts = lane_parts(block_ref.shape[0], bits)
    own = pltpu.make_async_copy(block_ref, out_ref.at[me], own_sem)
    own.start()
    greet(me, bits)
    copies = [{}, {}]
    waited = [set(), set()]
    for step in range(bits):
        for part, (start, size, order) in enumerate(parts):
            bit = order[bits - 1 - step]
            held = [0]
            for earlier in range(step):
                held = held + [p | 1 << order[bits - 1 - earlier] for p in held]
            for pattern in held:
                block = flipped(me, pattern, bits)
                if pattern:
                    if pattern not in waited[part]:
                        copies[part][pattern].wait_recv()
                        waited[part].add(pattern)
                    source = out_ref.at[block, pl.ds(start, size)]
                else:
                    source = block_ref.at[pl.ds(start, size)]
                slot = pattern | 1 << bit
                copy = pltpu.make_async_remote_copy(
                    src_ref=source,
                    dst_ref=out_ref.at[block, pl.ds(start, size)],
                    send_sem=send_sem.at[part, slot],
                    recv_sem=recv_sem.at[part, slot],
                    device_id={"ctx": flipped(me, 1 << bit, bits)},
                    device_id_type=pl.DeviceIdType.MESH,
                )
                copy.start()
                copies[part][slot] = copy
    for part in range(2):
        for slot, copy in copies[part].items():
            if slot not in waited[part]:
                copy.wait_recv()
            copy.wait_send()
    own.wait()


def gather_blocks(block, collective_id):
    shards = lax.axis_size("ctx")
    bits = shards.bit_length() - 1
    return pl.pallas_call(
        lambda *refs: gather_kernel(bits, *refs),
        out_shape=jax.ShapeDtypeStruct((shards,) + block.shape, block.dtype),
        in_specs=[pl.BlockSpec(memory_space=pltpu.VMEM)],
        out_specs=pl.BlockSpec(memory_space=pltpu.VMEM),
        scratch_shapes=[
            pltpu.SemaphoreType.DMA((2, shards)),
            pltpu.SemaphoreType.DMA((2, shards)),
            pltpu.SemaphoreType.DMA,
        ],
        compiler_params=pltpu.CompilerParams(collective_id=collective_id, has_side_effects=True),
        name="gather_blocks",
    )(block)


def scatter_kernel(bits, blocks_ref, out_ref, outbox, inbox, send_sem, recv_sem):
    me = lax.axis_index("ctx")
    shards = 1 << bits
    parts = lane_parts(blocks_ref.shape[1], bits)
    greet(me, bits)
    arrived = [{p: [] for p in range(shards)} for _ in parts]
    pending = [{}, {}]
    finished = [set(), set()]
    sent = []
    next_slot = [0, 0]

    def total(part, pattern):
        start, size, _ = parts[part]
        value = blocks_ref[flipped(me, pattern, bits), pl.ds(start, size), :].astype(jnp.float32)
        for slot in arrived[part][pattern]:
            if slot not in finished[part]:
                pending[part][slot].wait_recv()
                finished[part].add(slot)
            value = value + inbox[slot, pl.ds(start, size), :].astype(jnp.float32)
        return value

    for step in range(bits):
        fresh = []
        for part, (start, size, order) in enumerate(parts):
            bit = order[step]
            done_mask = sum(1 << b for b in order[:step])
            for pattern in range(shards):
                if pattern & done_mask or not pattern >> bit & 1:
                    continue
                slot = next_slot[part]
                next_slot[part] += 1
                if step:
                    outbox[slot, pl.ds(start, size), :] = total(part, pattern).astype(outbox.dtype)
                    source = outbox.at[slot, pl.ds(start, size)]
                else:
                    source = blocks_ref.at[flipped(me, pattern, bits), pl.ds(start, size)]
                copy = pltpu.make_async_remote_copy(
                    src_ref=source,
                    dst_ref=inbox.at[slot, pl.ds(start, size)],
                    send_sem=send_sem.at[part, slot],
                    recv_sem=recv_sem.at[part, slot],
                    device_id={"ctx": flipped(me, 1 << bit, bits)},
                    device_id_type=pl.DeviceIdType.MESH,
                )
                copy.start()
                pending[part][slot] = copy
                sent.append(copy)
                fresh.append((part, pattern ^ 1 << bit, slot))
        for part, pattern, slot in fresh:
            arrived[part][pattern].append(slot)
    for part, (start, size, _) in enumerate(parts):
        out_ref[pl.ds(start, size), :] = total(part, 0)
    for copy in sent:
        copy.wait_send()


def scatter_sum(blocks, collective_id):
    shards = lax.axis_size("ctx")
    bits = shards.bit_length() - 1
    return pl.pallas_call(
        lambda *refs: scatter_kernel(bits, *refs),
        out_shape=jax.ShapeDtypeStruct(blocks.shape[1:], jnp.float32),
        in_specs=[pl.BlockSpec(memory_space=pltpu.VMEM)],
        out_specs=pl.BlockSpec(memory_space=pltpu.VMEM),
        scratch_shapes=[
            pltpu.VMEM(blocks.shape, blocks.dtype),
            pltpu.VMEM(blocks.shape, blocks.dtype),
            pltpu.SemaphoreType.DMA((2, shards)),
            pltpu.SemaphoreType.DMA((2, shards)),
        ],
        compiler_params=pltpu.CompilerParams(collective_id=collective_id, has_side_effects=True),
        name="scatter_sum",
    )(blocks)


def local(
    queries,
    own_key,
    own_value,
    cache_keys,
    cache_values,
    prefix_of_row,
    context_len,
    hidden_in,
    w_out,
    norm_gain,
    expert_ids,
    route_weights,
    gate_up_codes,
    gate_up_scales,
    down_codes,
    down_scales,
):
    shards = lax.axis_size("ctx")
    device = lax.axis_index("ctx")
    head_size = HD
    local_rows = queries.shape[0]
    key_groups = own_key.shape[1] // head_size
    per_group = queries.shape[1] // own_key.shape[1]
    head_count = key_groups * per_group
    ctx_local = cache_keys.shape[1]
    key_width = cache_keys.shape[2]
    score_scale = 1.0 / math.sqrt(head_size)
    block_prefix = prefix_of_row.reshape(-1, CAND)[:, 0]
    prefix_count = block_prefix.shape[0]
    group_size = CAND // local_rows
    group_bits = group_size.bit_length() - 1
    prefix_bits = (shards // group_size).bit_length() - 1
    group_index = device // group_size
    member = device % group_size
    relay = jnp.concatenate(
        [jnp.take(cache_keys, block_prefix, axis=0), jnp.take(cache_values, block_prefix, axis=0)],
        axis=-1,
    )
    relay_shape = relay.shape
    for bit in range(prefix_bits):
        low = 1 << bit
        view = relay.reshape((relay_shape[0] // (2 * low), 2, low) + relay_shape[1:])
        own_bit = group_index // low % 2
        sent = lax.dynamic_index_in_dim(view, 1 - own_bit, 1, False)
        got = swapped(sent, "ctx", group_bits + bit)
        view = lax.dynamic_update_index_in_dim(view, got, 1 - own_bit, 1)
        relay = view.reshape(relay_shape)
    held = queries
    for bit in range(group_bits):
        other = swapped(held, "ctx", bit)
        upper = device // (1 << bit) % 2
        held = jnp.where(
            upper == 0, jnp.concatenate([held, other], 0), jnp.concatenate([other, held], 0)
        )
    length = jnp.take(context_len, jnp.take(block_prefix, group_index))
    source_block = jnp.arange(prefix_count, dtype=jnp.int32) * group_size + member
    position = source_block[:, None] * ctx_local + jnp.arange(ctx_local, dtype=jnp.int32)[None, :]
    is_valid = (position < length)[None]
    query_heads = held.reshape(1, CAND, key_groups, per_group, head_size)
    key_heads = relay[..., :key_width].reshape(1, prefix_count, ctx_local, key_groups, head_size)
    value_heads = relay[..., key_width:].reshape(1, prefix_count, ctx_local, key_groups, head_size)
    block_max, block_total, block_out = block_partials(
        query_heads, key_heads, value_heads, is_valid, score_scale
    )
    block_max = block_max.reshape(CAND, head_count, prefix_count)
    block_total = block_total.reshape(CAND, head_count, prefix_count)
    block_out = block_out.reshape(CAND, head_count, prefix_count, head_size)
    state = fold_blocks(block_max, block_total, block_out)
    for bit in reversed(range(group_bits)):
        own_bit = device // (1 << bit) % 2
        parts = tuple((item.reshape((2, item.shape[0] // 2) + item.shape[1:]) for item in state))
        sent = tuple((lax.dynamic_index_in_dim(item, 1 - own_bit, 0, False) for item in parts))
        kept = tuple((lax.dynamic_index_in_dim(item, own_bit, 0, False) for item in parts))
        got = swapped(sent, "ctx", bit)
        state = merge_pair(kept, got)
    merged_top, merged_numer, merged_denom = state
    own_heads = queries.reshape(local_rows, key_groups, per_group, head_size)
    own_keys = own_key.reshape(local_rows, key_groups, head_size)
    own_score = (
        jnp.einsum(
            "rgqd,rgd->rgq", own_heads, own_keys, preferred_element_type=jnp.float32
        ).reshape(local_rows, head_count)
        * score_scale
    )
    top_score = jnp.maximum(merged_top, own_score)
    block_scale = jnp.exp(merged_top - top_score)
    own_weight = jnp.exp(own_score - top_score)
    own_term = own_value.reshape(local_rows, key_groups, 1, head_size).astype(
        jnp.float32
    ) * own_weight.reshape(local_rows, key_groups, per_group, 1)
    numerator_all = merged_numer * block_scale[..., None] + own_term.reshape(
        local_rows, head_count, head_size
    )
    denominator = merged_denom * block_scale + own_weight
    attended = (numerator_all / denominator[..., None]).reshape(local_rows, -1).astype(jnp.bfloat16)
    feature_width = hidden_in.shape[1]
    lanes = feature_width // 128
    head_rows = lax.all_to_all(attended, "ctx", split_axis=1, concat_axis=0, tiled=True)
    partial = jnp.dot(head_rows, w_out, preferred_element_type=jnp.float32).astype(jnp.bfloat16)
    projected = scatter_sum(partial.reshape(shards, local_rows * lanes, 128), 1).reshape(
        local_rows, feature_width
    )
    mixed_rows = hidden_in.astype(jnp.float32) + projected
    attention_out = mixed_rows.astype(jnp.bfloat16)
    mean_square = jnp.mean(mixed_rows * mixed_rows, axis=-1, keepdims=True)
    normed = (mixed_rows * lax.rsqrt(mean_square + EPSILON) * norm_gain).astype(jnp.bfloat16)
    experts_all = shards // 2
    chosen = expert_ids[:, :, None] == jnp.arange(experts_all, dtype=jnp.int32)[None, None, :]
    dense = jnp.sum(jnp.where(chosen, route_weights[:, :, None], 0.0), axis=1)
    coarse = lax.reduce_precision(dense, exponent_bits=8, mantissa_bits=7)
    fine = dense - coarse
    weight_cols = jnp.concatenate([coarse, fine], axis=1).astype(jnp.bfloat16)
    weight_lanes = -(-weight_cols.shape[1] // 128)
    weight_cols = jnp.pad(weight_cols, ((0, 0), (0, weight_lanes * 128 - weight_cols.shape[1])))
    weight_block = weight_cols.reshape(local_rows * weight_lanes, 128)
    weight_block = jnp.pad(weight_block, ((0, -weight_block.shape[0] % 16), (0, 0)))
    block = jnp.concatenate([normed.reshape(local_rows * lanes, 128), weight_block], axis=0)
    gate_up = dequantize(gate_up_codes[0], gate_up_scales[0])
    down_proj = dequantize(down_codes[0], down_scales[0])
    half_width = down_proj.shape[0]
    gathered = gather_blocks(block, 2)
    all_rows = shards * local_rows
    flat_rows = gathered[:, : local_rows * lanes].reshape(all_rows, feature_width)
    weight_all = gathered[
        :, local_rows * lanes : local_rows * lanes + local_rows * weight_lanes
    ].reshape(all_rows, weight_lanes * 128)
    column = jnp.arange(weight_lanes * 128, dtype=jnp.int32) % experts_all
    in_use = jnp.arange(weight_lanes * 128, dtype=jnp.int32) < 2 * experts_all
    is_mine = jnp.logical_and(column == device // 2, in_use)
    row_weight = jnp.sum(
        jnp.where(is_mine[None, :], weight_all.astype(jnp.float32), 0.0), axis=1, keepdims=True
    )
    projected_in = jnp.dot(flat_rows, gate_up, preferred_element_type=jnp.float32)
    activated = (jax.nn.silu(projected_in[:, :half_width]) * projected_in[:, half_width:]).astype(
        jnp.bfloat16
    )
    result = jnp.dot(activated, down_proj, preferred_element_type=jnp.float32)
    result = jnp.where(row_weight != 0.0, result * row_weight, 0.0).astype(jnp.bfloat16)
    expert_sum = scatter_sum(result.reshape(shards, local_rows * lanes, 128), 3).reshape(
        local_rows, feature_width
    )
    layer_out = (mixed_rows + expert_sum).astype(jnp.bfloat16)
    return (attention_out, layer_out)


def solution(mesh):
    return jax.shard_map(
        local,
        mesh=mesh,
        in_specs=(
            P(("replica", "ctx"), None),
            P(("replica", "ctx"), None),
            P(("replica", "ctx"), None),
            P("replica", "ctx", None),
            P("replica", "ctx", None),
            P("replica"),
            P("replica"),
            P(("replica", "ctx"), None),
            P("ctx", None),
            P(),
            P(("replica", "ctx"), None),
            P(("replica", "ctx"), None),
            P("ctx", None, None),
            P("ctx", None, None),
            P("ctx", None, None),
            P("ctx", None, None),
        ),
        out_specs=(P(("replica", "ctx"), None), P(("replica", "ctx"), None)),
        check_vma=False,
    )
```
